32 devices in a mesh: gx: 4 (over y, core), gy: 4 (over z), gz: 2 (over x).
Axes of the slice: x: 2, y: 2, z: 4, core: 2. Of those that a mesh axis runs over, the one named last changes fastest.
Arguments:
- heat_level_grid: float32 [64, 256, 512], P('gz', 'gy', 'gx'), may hold values from -16 to 16, as said below
- interval_first_class: int32 [1], replicated, may hold values from 0 to 95
- interval_beyond_class: int32 [1], replicated, may hold values from 128 to 256
Outputs:
- magnitude: float32 [64, 256, 512], P('gz', 'gy', 'gx')
- histogram: float32 [256], replicated
- stats: float32 [4], replicated
The draws below stay inside these ranges and needn't reach their ends.
Inputs may be any that keep to these rules, and one draw needn't show every extreme that they name: `heat_level_grid`: each entry is a rough value times an amplitude that is constant on blocks of 8 x 4 x 4 cells (z, y, x) and varies over a factor of 16 between blocks.
All inputs are finite; a program needn't handle non-finite values.
Results may differ from the reference program's by a relative error of at most 0.0003.
Values sent between devices are 32-bit elements; how exact they have to be, the bound alone decides.
A program may use at most 64 MiB of HBM per device.

```python
import math
import jax
import jax.numpy as jnp

BINS = 256
NX = 512
NY = 256
NZ = 64


def draw_heat_level_grid(key, part):
    first_key, second_key = jax.random.split(jax.random.fold_in(key, 11))
    coarse = jax.random.uniform(first_key, (NZ // 8, NY // 4, NX // 4), jnp.float32, math.log(0.25), math.log(4.0))
    amplitude = jnp.exp(coarse)
    amplitude = jnp.repeat(jnp.repeat(jnp.repeat(amplitude, 8, axis=0), 4, axis=1), 4, axis=2)
    noise = jnp.clip(jax.random.normal(second_key, (NZ, NY, NX), jnp.float32), -4.0, 4.0)
    return (amplitude * noise).astype(jnp.float32)


def setup_inputs(seed: int = 0) -> dict:
    key_list = jax.random.split(jax.random.key(seed), 4)
    return {
        "heat_level_grid": draw_heat_level_grid(jax.random.fold_in(key_list[3], 71), 0),
        "interval_first_class": jax.random.randint(key_list[1], (1,), 0, 96).astype(jnp.int32),
        "interval_beyond_class": jax.random.randint(key_list[2], (1,), 128, BINS + 1).astype(jnp.int32),
    }


stencil_coefficients = (0.8, -0.2, 4.0 / 105.0, -1.0 / 280.0)
grad_range = 12.0

def directional_rate(field, direction_length_count):
    running = jnp.zeros_like(field)
    for offset, coefficient in enumerate(stencil_coefficients, start=1):
        running = running + coefficient * (jnp.roll(field, -offset, direction_length_count) - jnp.roll(field, offset, direction_length_count))
    return running

def reference(heat_level_grid, interval_first_class, interval_beyond_class):
    slope_norm_square = jnp.zeros_like(heat_level_grid)
    for direction_length_count in range(3):
        slope_in_direction = directional_rate(heat_level_grid, direction_length_count)
        slope_norm_square = slope_norm_square + slope_in_direction * slope_in_direction
    magnitude = jnp.sqrt(slope_norm_square + 1.0) - 1.0
    position = jnp.clip(magnitude * (BINS / grad_range), 0.5, BINS - 0.5)
    low_bin = jnp.minimum(jnp.floor(position - 0.5), BINS - 2).astype(jnp.int32)
    fraction = position - 0.5 - low_bin.astype(position.dtype)
    flat_low = low_bin.ravel()
    flat_frac = fraction.ravel()
    counts = jax.ops.segment_sum(1.0 - flat_frac, flat_low, BINS) + jax.ops.segment_sum(flat_frac, flat_low + 1, BINS)
    total_cells = NX * NY * NZ
    histogram = counts * (BINS / total_cells)
    lower_edge = interval_first_class[0]
    upper_edge = interval_beyond_class[0]
    high_bin = low_bin + 1
    inside_low = (low_bin >= lower_edge) & (low_bin < upper_edge)
    inside_high = (high_bin >= lower_edge) & (high_bin < upper_edge)
    weight = jnp.where(inside_low, 1.0 - fraction, 0.0) + jnp.where(inside_high, fraction, 0.0)
    lowest = jnp.min(magnitude + grad_range * (1.0 - weight))
    highest = jnp.max(weight * magnitude)
    weighted_sum = jnp.sum(weight * magnitude) / total_cells
    weighted_count = jnp.sum(weight) / total_cells
    stats = jnp.stack([lowest, highest, weighted_sum, weighted_count])
    return (magnitude, histogram, stats)
```

```python
import functools

import jax
import jax.numpy as jnp
from jax import lax
from jax.experimental import pallas as pl
from jax.experimental.pallas import tpu as pltpu
from jax.sharding import PartitionSpec as P

BINS = 256
FINE = 32
COARSE = BINS // FINE
GROUPS = 8
RANGE = 12.0
COEFS = (0.8, -0.2, 4.0 / 105.0, -1.0 / 280.0)
SCALE = 840.0
TAPS = (672.0, -168.0, 32.0, -3.0)
MESH = pl.DeviceIdType.MESH
F32 = jnp.float32
BF16 = jnp.bfloat16
UNROLL = 2


def tap(distance):
    value = jnp.zeros(distance.shape, F32)
    for k, t in enumerate(TAPS, start=1):
        value = jnp.where(distance == k, t, value)
        value = jnp.where(distance == -k, -t, value)
    return value


def kernel(
    sizes,
    first_ref,
    beyond_ref,
    x_ref,
    mag_ref,
    hist_ref,
    stat_ref,
    ext,
    mag,
    packed,
    from_left,
    from_right,
    band,
    rim_band,
    rim_part,
    acc,
    gather,
    in_sem,
    out_sem,
    send_sem,
    recv_sem,
    ready_y,
    ready_z,
    all_send,
    all_recv,
):
    names = ("gx", "gy", "gz")
    nz, ny, nx = x_ref.shape
    where = {a: lax.axis_index(a) for a in names}
    total = sizes["gx"] * sizes["gy"] * sizes["gz"]

    loads = [
        pltpu.make_async_copy(
            x_ref.at[pl.ds(a, b)], ext.at[pl.ds(4 + a, b), pl.ds(8, ny)], in_sem.at[i]
        )
        for i, (a, b) in enumerate(((0, nz // 2), (nz // 2, nz - nz // 2)))
    ]
    for c in loads:
        c.start()

    def others(axis):
        n = sizes[axis]
        return [lax.rem(where[axis] + d, n) for d in range(1, n)]

    barrier = pltpu.get_barrier_semaphore()
    greeted = 0
    for a in names:
        for other in others(a):
            pl.semaphore_signal(barrier, inc=1, device_id={a: other}, device_id_type=MESH)
            greeted += 1

    row = lax.broadcasted_iota(jnp.int32, (128, 128), 0)
    col = lax.broadcasted_iota(jnp.int32, (128, 128), 1)
    diag = tap(row - col).astype(BF16)
    band[0:128, :] = diag
    band[128:256, :] = diag
    r16 = lax.broadcasted_iota(jnp.int32, (16, 128), 0)
    l16 = lax.broadcasted_iota(jnp.int32, (16, 128), 1)
    m16 = lax.rem(r16, 8)
    place = jnp.where(m16 < 4, m16 - 4, 124 + m16)
    rim_tap = tap(place - l16)
    even = jnp.where(r16 < 8, rim_tap, 0.0).astype(BF16)
    odd = jnp.where(r16 >= 8, rim_tap, 0.0).astype(BF16)
    rim_band[...] = jnp.zeros(rim_band.shape, BF16)
    for j in range(16):
        tile = odd if j % 2 else even
        base = (j // 2) * 16
        rim_band[base : base + 16, 128 * j : 128 * (j + 1)] = tile
        rim_band[128 + base : 144 + base, 128 * j : 128 * (j + 1)] = tile
    acc[...] = jnp.zeros(acc.shape, F32)

    for c in loads:
        c.wait()

    planes = nz // 16
    lane = lax.broadcasted_iota(jnp.int32, (128, 128), 1)
    rims = None
    for j in range(16):
        block = ext[4 + planes * j : 4 + planes * (j + 1), 8 : 8 + ny, :].reshape(planes * ny, 128)
        turned = pltpu.roll(block, (8 * j + 4) % 128, 1)
        rims = turned if rims is None else jnp.where(lane >= 8 * j, turned, rims)
    packed[...] = rims

    pl.semaphore_wait(barrier, greeted)

    def up(a):
        return {a: lax.rem(where[a] + 1, sizes[a])}

    def down(a):
        return {a: lax.rem(where[a] + sizes[a] - 1, sizes[a])}

    def remote(src, dst, i, device):
        return pltpu.make_async_remote_copy(
            src_ref=src,
            dst_ref=dst,
            send_sem=send_sem.at[i],
            recv_sem=recv_sem.at[i],
            device_id=device,
            device_id_type=MESH,
        )

    own = pl.ds(4, nz)
    wide = pl.ds(8, ny)
    z_low = remote(ext.at[pl.ds(nz, 4), wide], ext.at[pl.ds(0, 4), wide], 4, up("gz"))
    z_high = remote(ext.at[pl.ds(4, 4), wide], ext.at[pl.ds(nz + 4, 4), wide], 5, down("gz"))
    y_low = remote(ext.at[own, pl.ds(4 + ny, 4)], ext.at[own, pl.ds(4, 4)], 2, up("gy"))
    y_high = remote(ext.at[own, pl.ds(8, 4)], ext.at[own, pl.ds(8 + ny, 4)], 3, down("gy"))
    x_low = remote(packed, from_left, 0, up("gx"))
    x_high = remote(packed, from_right, 1, down("gx"))
    x_low.start()
    x_high.start()
    y_low.start()
    y_high.start()
    z_low.start()
    z_high.start()
    for other in others("gy"):
        pl.semaphore_signal(ready_y, inc=1, device_id={"gy": other}, device_id_type=MESH)

    x_low.wait()
    x_high.wait()
    rim = jnp.where(lax.rem(lane, 8) < 4, from_left[...], from_right[...])
    rim_hi = rim.astype(BF16)
    rim_lo = (rim - rim_hi.astype(F32)).astype(BF16)
    rim_part[...] = jnp.dot(
        jnp.concatenate([rim_hi, rim_lo], axis=1), rim_band[...], preferred_element_type=F32
    )
    y_low.wait()
    y_high.wait()

    lower = first_ref[0].astype(F32) - 1.0
    upper = beyond_ref[0].astype(F32)
    parity = jnp.where(lax.broadcasted_iota(jnp.int32, (16, 128), 0) >= 8, 1.0, 0.0)

    def twice(a):
        return jnp.concatenate([a, a], axis=0)

    def plane(z):
        here = ext[z + 4, 8 : 8 + ny, :]
        hi = here.astype(BF16)
        lo = (here - hi.astype(F32)).astype(BF16)
        gx = jnp.dot(jnp.concatenate([hi, lo], axis=1), band[...], preferred_element_type=F32)
        rows = pl.multiple_of(lax.rem(z, planes) * ny, ny)
        cols = pl.multiple_of((z // planes) * 128, 128)
        gx = (gx + rim_part[pl.ds(rows, ny), pl.ds(cols, 128)]) * (1.0 / SCALE)
        gy = None
        gz = None
        for k, c in enumerate(COEFS, start=1):
            y_term = c * (ext[z + 4, 8 + k : 8 + k + ny, :] - ext[z + 4, 8 - k : 8 - k + ny, :])
            z_term = c * (ext[z + 4 + k, 8 : 8 + ny, :] - ext[z + 4 - k, 8 : 8 + ny, :])
            gy = y_term if gy is None else gy + y_term
            gz = z_term if gz is None else gz + z_term
        m = jnp.sqrt(gz * gz + gy * gy + gx * gx + 1.0) - 1.0
        mag[z] = m
        q = jnp.clip(m * (BINS / RANGE), 0.5, BINS - 0.5) - 0.5
        low = jnp.minimum(jnp.floor(q), BINS - 2.0)
        frac = q - low
        w = jnp.clip(jnp.minimum(q - lower, upper - q), 0.0, 1.0)
        wm = w * m
        worst = m + RANGE * (1.0 - w)
        coarse = jnp.floor(low * (1.0 / FINE))
        fine = low - FINE * coarse
        frac_hi = frac.astype(BF16).astype(F32)
        frac_lo = frac - frac_hi
        left, right = [], []
        zero = jnp.zeros((16, 128), BF16)
        one = jnp.ones((16, 128), BF16)
        for i in range(ny // 8):
            s = slice(8 * i, 8 * i + 8)
            c2 = (twice(coarse[s]) - parity).astype(BF16)
            f2 = (twice(fine[s]) - parity).astype(BF16)
            h2 = twice(frac_hi[s]).astype(BF16)
            l2 = twice(frac_lo[s]).astype(BF16)
            ones, his, los = [], [], []
            for j in range(COARSE // 2):
                hit = c2 == jnp.asarray(2 * j, BF16)
                ones.append(jnp.where(hit, one, zero))
                his.append(jnp.where(hit, h2, zero))
                los.append(jnp.where(hit, l2, zero))
            left.append(jnp.concatenate(ones + his + los, axis=0))
            right.append(
                jnp.concatenate(
                    [jnp.where(f2 == jnp.asarray(2 * j, BF16), one, zero) for j in range(FINE // 2)], axis=0
                )
            )
        fold = lambda op, a: functools.reduce(op, [a[8 * i : 8 * i + 8] for i in range(ny // 8)])
        return left, right, fold(jnp.add, wm), fold(jnp.add, w), fold(jnp.maximum, wm), fold(jnp.minimum, worst)

    def several(zs, carry):
        left, right = [], []
        s, n, hi, lo = carry
        for z in zs:
            l, r, ps, pn, phi, plo = plane(z)
            left += l
            right += r
            s, n, hi, lo = s + ps, n + pn, jnp.maximum(hi, phi), jnp.minimum(lo, plo)
        acc[...] += lax.dot_general(
            jnp.concatenate(left, axis=1),
            jnp.concatenate(right, axis=1),
            (((1,), (1,)), ((), ())),
            preferred_element_type=F32,
        )
        return s, n, hi, lo

    zeros = jnp.zeros((8, 128), F32)
    carry = (zeros, zeros, zeros, jnp.full((8, 128), 3.0e38, F32))
    inner = (nz - 8) // UNROLL
    carry = lax.fori_loop(
        0, inner, lambda t, c: several([4 + t * UNROLL + u for u in range(UNROLL)], c), carry
    )
    z_low.wait()
    z_high.wait()
    pl.semaphore_wait(ready_y, sizes["gy"] - 1)
    for other in others("gz"):
        pl.semaphore_signal(ready_z, inc=1, device_id={"gz": other}, device_id_type=MESH)
    middle = pltpu.make_async_copy(mag.at[pl.ds(4, nz - 8)], mag_ref.at[pl.ds(4, nz - 8)], out_sem.at[0])
    middle.start()

    def edge(t, c):
        z = t * UNROLL
        z = z + (z // 4) * (nz - 8)
        return several([z + u for u in range(UNROLL)], c)

    wsum, wcount, highest, lowest = lax.fori_loop(0, 8 // UNROLL, edge, carry)

    span = COARSE * GROUPS
    rows = lax.broadcasted_iota(jnp.int32, (span, FINE * GROUPS), 0)
    cols = lax.broadcasted_iota(jnp.int32, (span, FINE * GROUPS), 1)
    keep = lax.rem(rows, GROUPS) == lax.rem(cols, GROUPS)

    def by_class(a):
        a = jnp.where(keep, a, 0.0)
        return jnp.sum(a.reshape(COARSE, GROUPS, FINE * GROUPS), axis=1)

    count = by_class(acc[0:span, :])
    part = by_class(acc[span : 2 * span, :] + acc[2 * span : 3 * span, :])
    from_row = lax.broadcasted_iota(jnp.int32, (FINE * GROUPS, 128), 0) // GROUPS
    to_lane = lax.rem(lax.broadcasted_iota(jnp.int32, (FINE * GROUPS, 128), 1), FINE)
    spread = jnp.where(from_row == to_lane, 1.0, 0.0)
    both = jnp.dot(
        jnp.concatenate([count, part], axis=0),
        spread,
        precision=lax.Precision.HIGHEST,
        preferred_element_type=F32,
    )
    r8 = lax.broadcasted_iota(jnp.int32, (16, 128), 0)
    l8 = lax.broadcasted_iota(jnp.int32, (16, 128), 1)
    both = jnp.where(lax.rem(r8, 4) == l8 // FINE, both, 0.0)
    quad = [jnp.sum(both[4 * i : 4 * i + 4], axis=0, keepdims=True) for i in range(4)]
    lane1 = lax.broadcasted_iota(jnp.int32, (1, 128), 1)
    turned = [pltpu.roll(quad[2], 1, 1), pltpu.roll(quad[3], 1, 1)]
    row0 = quad[0] - quad[2] + jnp.where(lane1 == 0, turned[1], turned[0])
    row1 = quad[1] - quad[3] + jnp.where(lane1 == 0, turned[0], turned[1])

    def all_of(op, a):
        return op(op(a, axis=0, keepdims=True), axis=1, keepdims=True)

    row2 = jnp.where(
        lane1 == 0,
        all_of(jnp.min, lowest),
        jnp.where(
            lane1 == 1,
            all_of(jnp.max, highest),
            jnp.where(lane1 == 2, all_of(jnp.sum, wsum), all_of(jnp.sum, wcount)),
        ),
    )
    me = (where["gx"] * sizes["gy"] + where["gy"]) * sizes["gz"] + where["gz"]
    gather[me] = jnp.concatenate([row0, row1, row2, jnp.zeros((1, 128), F32)], axis=0)

    pl.semaphore_wait(ready_z, sizes["gz"] - 1)

    def spread_out(t, c):
        other = lax.rem(me + t, total)
        pltpu.make_async_remote_copy(
            src_ref=gather.at[me],
            dst_ref=gather.at[me],
            send_sem=all_send,
            recv_sem=all_recv,
            device_id={
                "gx": other // (sizes["gy"] * sizes["gz"]),
                "gy": lax.rem(other // sizes["gz"], sizes["gy"]),
                "gz": lax.rem(other, sizes["gz"]),
            },
            device_id_type=MESH,
        ).start()
        return c

    lax.fori_loop(1, total, spread_out, 0)
    outer = [
        pltpu.make_async_copy(mag.at[pl.ds(a, 4)], mag_ref.at[pl.ds(a, 4)], out_sem.at[i])
        for i, a in ((1, 0), (2, nz - 4))
    ]
    for c in outer:
        c.start()
    rest = gather.at[pl.ds(0, total - 1)]
    every = pltpu.make_async_remote_copy(
        src_ref=rest,
        dst_ref=rest,
        send_sem=all_send,
        recv_sem=all_recv,
        device_id=up("gx"),
        device_id_type=MESH,
    )
    every.wait()
    parts = gather[...]
    summed = jnp.sum(parts, axis=0)
    smallest = jnp.min(parts, axis=0)
    largest = jnp.max(parts, axis=0)
    cells = nz * ny * nx * total
    hist_ref[...] = summed[0:2] * (BINS / cells)
    stat_ref[...] = jnp.where(
        lane1 == 0,
        smallest[2:3],
        jnp.where(lane1 == 1, largest[2:3], summed[2:3] * (1.0 / cells)),
    )
    middle.wait()
    for c in outer:
        c.wait()


def solution(mesh):
    sizes = dict(mesh.shape)
    total = sizes["gx"] * sizes["gy"] * sizes["gz"]

    def on_device(grid, first, beyond):
        nz, ny, nx = grid.shape
        vmem = pl.BlockSpec(memory_space=pltpu.VMEM)
        smem = pl.BlockSpec(memory_space=pltpu.SMEM)
        anywhere = pl.BlockSpec(memory_space=pl.ANY)
        packed_rows = nz * ny // 16
        magnitude, histogram, stats = pl.pallas_call(
            functools.partial(kernel, sizes),
            out_shape=(
                jax.ShapeDtypeStruct(grid.shape, F32),
                jax.ShapeDtypeStruct((2, 128), F32),
                jax.ShapeDtypeStruct((1, 128), F32),
            ),
            in_specs=[smem, smem, anywhere],
            out_specs=(anywhere, vmem, vmem),
            scratch_shapes=[
                pltpu.VMEM((nz + 8, ny + 16, nx), F32),
                pltpu.VMEM((nz, ny, nx), F32),
                pltpu.VMEM((packed_rows, 128), F32),
                pltpu.VMEM((packed_rows, 128), F32),
                pltpu.VMEM((packed_rows, 128), F32),
                pltpu.VMEM((256, 128), BF16),
                pltpu.VMEM((256, 2048), BF16),
                pltpu.VMEM((packed_rows, 2048), F32),
                pltpu.VMEM((3 * COARSE * GROUPS, FINE * GROUPS), F32),
                pltpu.VMEM((total, 4, 128), F32),
                pltpu.SemaphoreType.DMA((2,)),
                pltpu.SemaphoreType.DMA((3,)),
                pltpu.SemaphoreType.DMA((6,)),
                pltpu.SemaphoreType.DMA((6,)),
                pltpu.SemaphoreType.REGULAR,
                pltpu.SemaphoreType.REGULAR,
                pltpu.SemaphoreType.DMA,
                pltpu.SemaphoreType.DMA,
            ],
            compiler_params=pltpu.CompilerParams(
                collective_id=0, has_side_effects=True, vmem_limit_bytes=32 * 1024 * 1024
            ),
        )(first, beyond, grid)
        return magnitude, histogram.reshape(BINS), stats[0, 0:4]

    return jax.shard_map(
        on_device,
        mesh=mesh,
        in_specs=(P("gz", "gy", "gx"), P(), P()),
        out_specs=(P("gz", "gy", "gx"), P(), P()),
        check_vma=False,
    )
```

```python
import functools

import jax
import jax.numpy as jnp
from jax import lax
from jax.experimental import pallas as pl
from jax.experimental.pallas import tpu as pltpu
from jax.sharding import PartitionSpec as P

BINS = 256
FINE = 32
COARSE = BINS // FINE
GROUPS = 8
RANGE = 12.0
COEFS = (0.8, -0.2, 4.0 / 105.0, -1.0 / 280.0)
SCALE = 840.0
TAPS = (672.0, -168.0, 32.0, -3.0)
MESH = pl.DeviceIdType.MESH
F32 = jnp.float32
BF16 = jnp.bfloat16
UNROLL = 4
EDGE = 2


def tap(distance):
    value = jnp.zeros(distance.shape, F32)
    for k, t in enumerate(TAPS, start=1):
        value = jnp.where(distance == k, t, value)
        value = jnp.where(distance == -k, -t, value)
    return value


def kernel(
    sizes,
    first_ref,
    beyond_ref,
    x_ref,
    mag_ref,
    hist_ref,
    stat_ref,
    ext,
    packed,
    from_left,
    from_right,
    band,
    rim_band,
    rim_part,
    acc,
    gather,
    in_sem,
    send_sem,
    recv_sem,
    ready_y,
    ready_z,
    all_send,
    all_recv,
):
    names = ("gx", "gy", "gz")
    nz, ny, nx = x_ref.shape
    where = {a: lax.axis_index(a) for a in names}
    total = sizes["gx"] * sizes["gy"] * sizes["gz"]

    loads = [
        pltpu.make_async_copy(
            x_ref.at[pl.ds(a, b)], ext.at[pl.ds(4 + a, b), pl.ds(8, ny)], in_sem.at[i]
        )
        for i, (a, b) in enumerate(((0, nz // 2), (nz // 2, nz - nz // 2)))
    ]
    for c in loads:
        c.start()

    def others(axis):
        n = sizes[axis]
        return [lax.rem(where[axis] + d, n) for d in range(1, n)]

    ahead = {(a, d): lax.rem(where[a] + d, sizes[a]) for a in names for d in range(sizes[a])}
    barrier = pltpu.get_barrier_semaphore()
    greeted = 0
    for a in names:
        for other in others(a):
            pl.semaphore_signal(barrier, inc=1, device_id={a: other}, device_id_type=MESH)
            greeted += 1

    row = lax.broadcasted_iota(jnp.int32, (128, 128), 0)
    col = lax.broadcasted_iota(jnp.int32, (128, 128), 1)
    diag = tap(row - col).astype(BF16)
    band[0:128, :] = diag
    band[128:256, :] = diag
    r16 = lax.broadcasted_iota(jnp.int32, (16, 128), 0)
    l16 = lax.broadcasted_iota(jnp.int32, (16, 128), 1)
    m16 = lax.rem(r16, 8)
    place = jnp.where(m16 < 4, m16 - 4, 124 + m16)
    rim_tap = tap(place - l16)
    even = jnp.where(r16 < 8, rim_tap, 0.0).astype(BF16)
    odd = jnp.where(r16 >= 8, rim_tap, 0.0).astype(BF16)
    rim_band[...] = jnp.zeros(rim_band.shape, BF16)
    for j in range(16):
        tile = odd if j % 2 else even
        base = (j // 2) * 16
        rim_band[base : base + 16, 128 * j : 128 * (j + 1)] = tile
        rim_band[128 + base : 144 + base, 128 * j : 128 * (j + 1)] = tile
    acc[...] = jnp.zeros(acc.shape, F32)

    for c in loads:
        c.wait()

    planes = nz // 16
    lane = lax.broadcasted_iota(jnp.int32, (128, 128), 1)
    rims = None
    for j in range(16):
        block = ext[4 + planes * j : 4 + planes * (j + 1), 8 : 8 + ny, :].reshape(planes * ny, 128)
        turned = pltpu.roll(block, (8 * j + 4) % 128, 1)
        rims = turned if rims is None else jnp.where(lane >= 8 * j, turned, rims)
    packed[...] = rims

    pl.semaphore_wait(barrier, greeted)

    def up(a):
        return {a: lax.rem(where[a] + 1, sizes[a])}

    def down(a):
        return {a: lax.rem(where[a] + sizes[a] - 1, sizes[a])}

    def remote(src, dst, i, device):
        return pltpu.make_async_remote_copy(
            src_ref=src,
            dst_ref=dst,
            send_sem=send_sem.at[i],
            recv_sem=recv_sem.at[i],
            device_id=device,
            device_id_type=MESH,
        )

    own = pl.ds(4, nz)
    wide = pl.ds(8, ny)
    z_low = remote(ext.at[pl.ds(nz, 4), wide], ext.at[pl.ds(0, 4), wide], 4, up("gz"))
    z_high = remote(ext.at[pl.ds(4, 4), wide], ext.at[pl.ds(nz + 4, 4), wide], 5, down("gz"))
    y_low = remote(ext.at[own, pl.ds(4 + ny, 4)], ext.at[own, pl.ds(4, 4)], 2, up("gy"))
    y_high = remote(ext.at[own, pl.ds(8, 4)], ext.at[own, pl.ds(8 + ny, 4)], 3, down("gy"))
    x_low = remote(packed, from_left, 0, up("gx"))
    x_high = remote(packed, from_right, 1, down("gx"))
    x_low.start()
    x_high.start()
    y_low.start()
    y_high.start()
    z_low.start()
    z_high.start()
    for other in others("gy"):
        pl.semaphore_signal(ready_y, inc=1, device_id={"gy": other}, device_id_type=MESH)

    x_low.wait()
    x_high.wait()
    rim = jnp.where(lax.rem(lane, 8) < 4, from_left[...], from_right[...])
    rim_hi = rim.astype(BF16)
    rim_lo = (rim - rim_hi.astype(F32)).astype(BF16)
    rim_part[...] = jnp.dot(
        jnp.concatenate([rim_hi, rim_lo], axis=1), rim_band[...], preferred_element_type=F32
    )
    lower = first_ref[0].astype(F32) - 1.0
    upper = beyond_ref[0].astype(F32)
    parity = jnp.where(lax.broadcasted_iota(jnp.int32, (16, 128), 0) >= 8, 1.0, 0.0)

    def twice(a):
        return jnp.concatenate([a, a], axis=0)

    def rates(blocks):
        sides = []
        for z, t0, nt in blocks:
            here = ext[z + 4, 8 + 8 * t0 : 8 + 8 * (t0 + nt), :]
            hi = here.astype(BF16)
            lo = (here - hi.astype(F32)).astype(BF16)
            sides.append(jnp.concatenate([hi, lo], axis=1))
        return jnp.dot(jnp.concatenate(sides, axis=0), band[...], preferred_element_type=F32)

    def plane(z, t0, nt, gx):
        y0, n = 8 + 8 * t0, 8 * nt
        rows = pl.multiple_of(lax.rem(z, planes) * ny + 8 * t0, 8)
        cols = pl.multiple_of((z // planes) * 128, 128)
        gx = (gx + rim_part[pl.ds(rows, n), pl.ds(cols, 128)]) * (1.0 / SCALE)
        gy = None
        gz = None
        for k, c in enumerate(COEFS, start=1):
            y_term = c * (ext[z + 4, y0 + k : y0 + k + n, :] - ext[z + 4, y0 - k : y0 - k + n, :])
            z_term = c * (ext[z + 4 + k, y0 : y0 + n, :] - ext[z + 4 - k, y0 : y0 + n, :])
            gy = y_term if gy is None else gy + y_term
            gz = z_term if gz is None else gz + z_term
        m = jnp.sqrt(gz * gz + gy * gy + gx * gx + 1.0) - 1.0
        mag_ref[z, 8 * t0 : 8 * (t0 + nt), :] = m
        q = jnp.clip(m * (BINS / RANGE), 0.5, BINS - 0.5) - 0.5
        low = jnp.minimum(jnp.floor(q), BINS - 2.0)
        frac = q - low
        w = jnp.clip(jnp.minimum(q - lower, upper - q), 0.0, 1.0)
        wm = w * m
        worst = m + RANGE * (1.0 - w)
        coarse = jnp.floor(low * (1.0 / FINE))
        fine = low - FINE * coarse
        frac_hi = frac.astype(BF16).astype(F32)
        frac_lo = frac - frac_hi
        left, right = [], []
        zero = jnp.zeros((16, 128), BF16)
        one = jnp.ones((16, 128), BF16)
        for i in range(nt):
            s = slice(8 * i, 8 * i + 8)
            c2 = (twice(coarse[s]) - parity).astype(BF16)
            f2 = (twice(fine[s]) - parity).astype(BF16)
            h2 = twice(frac_hi[s]).astype(BF16)
            l2 = twice(frac_lo[s]).astype(BF16)
            ones, his, los = [], [], []
            for j in range(COARSE // 2):
                hit = c2 == jnp.asarray(2 * j, BF16)
                ones.append(jnp.where(hit, one, zero))
                his.append(jnp.where(hit, h2, zero))
                los.append(jnp.where(hit, l2, zero))
            left.append(jnp.concatenate(ones + his + los, axis=0))
            right.append(
                jnp.concatenate(
                    [jnp.where(f2 == jnp.asarray(2 * j, BF16), one, zero) for j in range(FINE // 2)], axis=0
                )
            )
        fold = lambda op, a: functools.reduce(op, [a[8 * i : 8 * i + 8] for i in range(nt)])
        return left, right, fold(jnp.add, wm), fold(jnp.add, w), fold(jnp.maximum, wm), fold(jnp.minimum, worst)

    def several(blocks, carry):
        left, right = [], []
        s, n, hi, lo = carry
        gx = rates(blocks)
        start = 0
        for z, t0, nt in blocks:
            l, r, ps, pn, phi, plo = plane(z, t0, nt, gx[start : start + 8 * nt])
            start += 8 * nt
            left += l
            right += r
            s, n, hi, lo = s + ps, n + pn, jnp.maximum(hi, phi), jnp.minimum(lo, plo)
        acc[...] += lax.dot_general(
            jnp.concatenate(left, axis=1),
            jnp.concatenate(right, axis=1),
            (((1,), (1,)), ((), ())),
            preferred_element_type=F32,
        )
        return s, n, hi, lo

    zeros = jnp.zeros((8, 128), F32)
    carry = (zeros, zeros, zeros, jnp.full((8, 128), 3.0e38, F32))
    tiles = ny // 8
    inner = (nz - 8) // UNROLL
    carry = lax.fori_loop(
        0, inner, lambda t, c: several([(4 + t * UNROLL + u, 1, tiles - 2) for u in range(UNROLL)], c), carry
    )
    y_low.wait()
    y_high.wait()
    ends = [(u, t0, 1) for u in range(8) for t0 in (0, tiles - 1)]
    carry = lax.fori_loop(
        0, (nz - 8) // 8, lambda t, c: several([(4 + t * 8 + u, a, b) for u, a, b in ends], c), carry
    )
    z_low.wait()
    z_high.wait()
    pl.semaphore_wait(ready_y, sizes["gy"] - 1)
    for other in others("gz"):
        pl.semaphore_signal(ready_z, inc=1, device_id={"gz": other}, device_id_type=MESH)

    def edge(t, c):
        z = t * EDGE
        z = z + (z // 4) * (nz - 8)
        return several([(z + u, 0, tiles) for u in range(EDGE)], c)

    wsum, wcount, highest, lowest = lax.fori_loop(0, 8 // EDGE, edge, carry)

    span = COARSE * GROUPS
    rows = lax.broadcasted_iota(jnp.int32, (span, FINE * GROUPS), 0)
    cols = lax.broadcasted_iota(jnp.int32, (span, FINE * GROUPS), 1)
    keep = lax.rem(rows, GROUPS) == lax.rem(cols, GROUPS)

    def by_class(a):
        a = jnp.where(keep, a, 0.0)
        return jnp.sum(a.reshape(COARSE, GROUPS, FINE * GROUPS), axis=1)

    count = by_class(acc[0:span, :])
    part = by_class(acc[span : 2 * span, :] + acc[2 * span : 3 * span, :])
    from_row = lax.broadcasted_iota(jnp.int32, (FINE * GROUPS, 128), 0) // GROUPS
    to_lane = lax.rem(lax.broadcasted_iota(jnp.int32, (FINE * GROUPS, 128), 1), FINE)
    spread = jnp.where(from_row == to_lane, 1.0, 0.0)
    both = jnp.dot(
        jnp.concatenate([count, part], axis=0),
        spread,
        precision=lax.Precision.HIGHEST,
        preferred_element_type=F32,
    )
    r8 = lax.broadcasted_iota(jnp.int32, (16, 128), 0)
    l8 = lax.broadcasted_iota(jnp.int32, (16, 128), 1)
    both = jnp.where(lax.rem(r8, 4) == l8 // FINE, both, 0.0)
    quad = [jnp.sum(both[4 * i : 4 * i + 4], axis=0, keepdims=True) for i in range(4)]
    lane1 = lax.broadcasted_iota(jnp.int32, (1, 128), 1)
    turned = [pltpu.roll(quad[2], 1, 1), pltpu.roll(quad[3], 1, 1)]
    row0 = quad[0] - quad[2] + jnp.where(lane1 == 0, turned[1], turned[0])
    row1 = quad[1] - quad[3] + jnp.where(lane1 == 0, turned[0], turned[1])

    def all_of(op, a):
        return op(op(a, axis=0, keepdims=True), axis=1, keepdims=True)

    row2 = jnp.where(
        lane1 == 0,
        all_of(jnp.min, lowest),
        jnp.where(
            lane1 == 1,
            all_of(jnp.max, highest),
            jnp.where(lane1 == 2, all_of(jnp.sum, wsum), all_of(jnp.sum, wcount)),
        ),
    )
    me = (where["gx"] * sizes["gy"] + where["gy"]) * sizes["gz"] + where["gz"]
    gather[me] = jnp.concatenate([row0, row1, row2, jnp.zeros((1, 128), F32)], axis=0)

    pl.semaphore_wait(ready_z, sizes["gz"] - 1)

    def spread_to(gx, gy, gz):
        pltpu.make_async_remote_copy(
            src_ref=gather.at[me],
            dst_ref=gather.at[me],
            send_sem=all_send,
            recv_sem=all_recv,
            device_id={"gx": gx, "gy": gy, "gz": gz},
            device_id_type=MESH,
        ).start()

    def spread_out(t, c):
        other = lax.rem(me + t, total)
        spread_to(
            other // (sizes["gy"] * sizes["gz"]),
            lax.rem(other // sizes["gz"], sizes["gy"]),
            lax.rem(other, sizes["gz"]),
        )
        return c

    if total > 64:
        lax.fori_loop(1, total, spread_out, 0)
    else:
        far = lambda n: sorted(range(n), key=lambda d: -min(d, n - d))
        for dy in far(sizes["gy"]):
            for dz in far(sizes["gz"]):
                for dx in far(sizes["gx"]):
                    if dx or dy or dz:
                        spread_to(*[ahead[a, d] for a, d in (("gx", dx), ("gy", dy), ("gz", dz))])
    rest = gather.at[pl.ds(0, total - 1)]
    every = pltpu.make_async_remote_copy(
        src_ref=rest,
        dst_ref=rest,
        send_sem=all_send,
        recv_sem=all_recv,
        device_id=up("gx"),
        device_id_type=MESH,
    )
    every.wait()
    parts = gather[...]
    summed = jnp.sum(parts, axis=0)
    smallest = jnp.min(parts, axis=0)
    largest = jnp.max(parts, axis=0)
    cells = nz * ny * nx * total
    hist_ref[...] = summed[0:2] * (BINS / cells)
    stat_ref[...] = jnp.where(
        lane1 == 0,
        smallest[2:3],
        jnp.where(lane1 == 1, largest[2:3], summed[2:3] * (1.0 / cells)),
    )[:, 0:4]


def finish(mag_ref, hist_ref, stat_ref, mag_out, hist_out, stat_out, sem):
    copy = pltpu.make_async_copy(mag_ref, mag_out, sem)
    copy.start()
    hist_out[...] = hist_ref[...]
    stat_out[...] = stat_ref[...]
    copy.wait()


def solution(mesh):
    sizes = dict(mesh.shape)
    total = sizes["gx"] * sizes["gy"] * sizes["gz"]

    def on_device(grid, first, beyond):
        nz, ny, nx = grid.shape
        vmem = pl.BlockSpec(memory_space=pltpu.VMEM)
        hbm = pl.BlockSpec(memory_space=pltpu.HBM)
        packed_rows = nz * ny // 16
        magnitude, histogram, stats = pl.pallas_call(
            functools.partial(kernel, sizes),
            out_shape=(
                jax.ShapeDtypeStruct(grid.shape, F32),
                jax.ShapeDtypeStruct((2, 128), F32),
                jax.ShapeDtypeStruct((1, 4), F32),
            ),
            in_specs=[pl.BlockSpec(memory_space=pltpu.SMEM), pl.BlockSpec(memory_space=pltpu.SMEM), hbm],
            out_specs=(vmem, vmem, vmem),
            scratch_shapes=[
                pltpu.VMEM((nz + 8, ny + 16, nx), F32),
                pltpu.VMEM((packed_rows, 128), F32),
                pltpu.VMEM((packed_rows, 128), F32),
                pltpu.VMEM((packed_rows, 128), F32),
                pltpu.VMEM((256, 128), BF16),
                pltpu.VMEM((256, 2048), BF16),
                pltpu.VMEM((packed_rows, 2048), F32),
                pltpu.VMEM((3 * COARSE * GROUPS, FINE * GROUPS), F32),
                pltpu.VMEM((total, 4, 128), F32),
                pltpu.SemaphoreType.DMA((2,)),
                pltpu.SemaphoreType.DMA((6,)),
                pltpu.SemaphoreType.DMA((6,)),
                pltpu.SemaphoreType.REGULAR,
                pltpu.SemaphoreType.REGULAR,
                pltpu.SemaphoreType.DMA,
                pltpu.SemaphoreType.DMA,
            ],
            compiler_params=pltpu.CompilerParams(
                collective_id=0, has_side_effects=True, vmem_limit_bytes=32768 * 1024
            ),
        )(first, beyond, grid)
        magnitude, histogram, stats = pl.pallas_call(
            finish,
            out_shape=(
                jax.ShapeDtypeStruct(grid.shape, F32),
                jax.ShapeDtypeStruct((2, 128), F32),
                jax.ShapeDtypeStruct((1, 4), F32),
            ),
            in_specs=[vmem, vmem, vmem],
            out_specs=(hbm, vmem, vmem),
            scratch_shapes=[pltpu.SemaphoreType.DMA],
            compiler_params=pltpu.CompilerParams(vmem_limit_bytes=4 * 1024 * 1024),
        )(magnitude, histogram, stats)
        return magnitude, histogram.reshape(BINS), stats.reshape(4)

    return jax.shard_map(
        on_device,
        mesh=mesh,
        in_specs=(P("gz", "gy", "gx"), P(), P()),
        out_specs=(P("gz", "gy", "gx"), P(), P()),
        check_vma=False,
    )
```

```python
import functools

import jax
import jax.numpy as jnp
from jax import lax
from jax.experimental import pallas as pl
from jax.experimental.pallas import tpu as pltpu
from jax.sharding import PartitionSpec as P

BINS = 256
FINE = 32
COARSE = BINS // FINE
GROUPS = 8
RANGE = 12.0
COEFS = (0.8, -0.2, 4.0 / 105.0, -1.0 / 280.0)
SCALE = 840.0
TAPS = (672.0, -168.0, 32.0, -3.0)
MESH = pl.DeviceIdType.MESH
F32 = jnp.float32
BF16 = jnp.bfloat16
UNROLL = 8
EDGE = 4


def tap(distance):
    value = jnp.zeros(distance.shape, F32)
    for k, t in enumerate(TAPS, start=1):
        value = jnp.where(distance == k, t, value)
        value = jnp.where(distance == -k, -t, value)
    return value


def kernel(
    sizes,
    first_ref,
    beyond_ref,
    x_ref,
    mag_ref,
    hist_ref,
    stat_ref,
    ext,
    packed,
    from_left,
    from_right,
    band,
    rim_band,
    rim_part,
    acc,
    gather,
    in_sem,
    send_sem,
    recv_sem,
    ready_y,
    ready_z,
    all_send,
    all_recv,
):
    names = ("gx", "gy", "gz")
    nz, ny, nx = x_ref.shape
    where = {a: lax.axis_index(a) for a in names}
    total = sizes["gx"] * sizes["gy"] * sizes["gz"]

    loads = [
        pltpu.make_async_copy(
            x_ref.at[pl.ds(a, b)], ext.at[pl.ds(4 + a, b), pl.ds(8, ny)], in_sem.at[i]
        )
        for i, (a, b) in enumerate(((0, nz // 2), (nz // 2, nz - nz // 2)))
    ]
    for c in loads:
        c.start()

    def others(axis):
        n = sizes[axis]
        return [lax.rem(where[axis] + d, n) for d in range(1, n)]

    ahead = {(a, d): lax.rem(where[a] + d, sizes[a]) for a in names for d in range(sizes[a])}
    barrier = pltpu.get_barrier_semaphore()
    greeted = 0
    for a in names:
        for other in others(a):
            pl.semaphore_signal(barrier, inc=1, device_id={a: other}, device_id_type=MESH)
            greeted += 1

    row = lax.broadcasted_iota(jnp.int32, (128, 128), 0)
    col = lax.broadcasted_iota(jnp.int32, (128, 128), 1)
    diag = tap(row - col).astype(BF16)
    band[0:128, :] = diag
    band[128:256, :] = diag
    r16 = lax.broadcasted_iota(jnp.int32, (16, 128), 0)
    l16 = lax.broadcasted_iota(jnp.int32, (16, 128), 1)
    m16 = lax.rem(r16, 8)
    place = jnp.where(m16 < 4, m16 - 4, 124 + m16)
    rim_tap = tap(place - l16)
    even = jnp.where(r16 < 8, rim_tap, 0.0).astype(BF16)
    odd = jnp.where(r16 >= 8, rim_tap, 0.0).astype(BF16)
    rim_band[...] = jnp.zeros(rim_band.shape, BF16)
    for j in range(16):
        tile = odd if j % 2 else even
        base = (j // 2) * 16
        rim_band[base : base + 16, 128 * j : 128 * (j + 1)] = tile
        rim_band[128 + base : 144 + base, 128 * j : 128 * (j + 1)] = tile
    acc[...] = jnp.zeros(acc.shape, F32)

    for c in loads:
        c.wait()

    planes = nz // 16
    lane = lax.broadcasted_iota(jnp.int32, (128, 128), 1)
    rims = None
    for j in range(16):
        block = ext[4 + planes * j : 4 + planes * (j + 1), 8 : 8 + ny, :].reshape(planes * ny, 128)
        turned = pltpu.roll(block, (8 * j + 4) % 128, 1)
        rims = turned if rims is None else jnp.where(lane >= 8 * j, turned, rims)
    packed[...] = rims

    pl.semaphore_wait(barrier, greeted)

    def up(a):
        return {a: lax.rem(where[a] + 1, sizes[a])}

    def down(a):
        return {a: lax.rem(where[a] + sizes[a] - 1, sizes[a])}

    def remote(src, dst, i, device):
        return pltpu.make_async_remote_copy(
            src_ref=src,
            dst_ref=dst,
            send_sem=send_sem.at[i],
            recv_sem=recv_sem.at[i],
            device_id=device,
            device_id_type=MESH,
        )

    own = pl.ds(4, nz)
    wide = pl.ds(8, ny)
    z_low = remote(ext.at[pl.ds(nz, 4), wide], ext.at[pl.ds(0, 4), wide], 4, up("gz"))
    z_high = remote(ext.at[pl.ds(4, 4), wide], ext.at[pl.ds(nz + 4, 4), wide], 5, down("gz"))
    y_low = remote(ext.at[own, pl.ds(4 + ny, 4)], ext.at[own, pl.ds(4, 4)], 2, up("gy"))
    y_high = remote(ext.at[own, pl.ds(8, 4)], ext.at[own, pl.ds(8 + ny, 4)], 3, down("gy"))
    x_low = remote(packed, from_left, 0, up("gx"))
    x_high = remote(packed, from_right, 1, down("gx"))
    x_low.start()
    x_high.start()
    y_low.start()
    y_high.start()
    z_low.start()
    z_high.start()
    for other in others("gy"):
        pl.semaphore_signal(ready_y, inc=1, device_id={"gy": other}, device_id_type=MESH)

    x_low.wait()
    x_high.wait()
    rim = jnp.where(lax.rem(lane, 8) < 4, from_left[...], from_right[...])
    rim_hi = rim.astype(BF16)
    rim_lo = (rim - rim_hi.astype(F32)).astype(BF16)
    rim_part[...] = jnp.dot(
        jnp.concatenate([rim_hi, rim_lo], axis=1), rim_band[...], preferred_element_type=F32
    )
    lower = first_ref[0].astype(F32) - 1.0
    upper = beyond_ref[0].astype(F32)
    parity = jnp.where(lax.broadcasted_iota(jnp.int32, (16, 128), 0) >= 8, 1.0, 0.0)

    def twice(a):
        return jnp.concatenate([a, a], axis=0)

    def rates(blocks):
        sides = []
        for z, t0, nt in blocks:
            here = ext[z + 4, 8 + 8 * t0 : 8 + 8 * (t0 + nt), :]
            hi = here.astype(BF16)
            lo = (here - hi.astype(F32)).astype(BF16)
            sides.append(jnp.concatenate([hi, lo], axis=1))
        return jnp.dot(jnp.concatenate(sides, axis=0), band[...], preferred_element_type=F32)

    def plane(z, t0, nt, gx):
        y0, n = 8 + 8 * t0, 8 * nt
        rows = pl.multiple_of(lax.rem(z, planes) * ny + 8 * t0, 8)
        cols = pl.multiple_of((z // planes) * 128, 128)
        gx = (gx + rim_part[pl.ds(rows, n), pl.ds(cols, 128)]) * (1.0 / SCALE)
        gy = None
        gz = None
        for k, c in enumerate(COEFS, start=1):
            y_term = c * (ext[z + 4, y0 + k : y0 + k + n, :] - ext[z + 4, y0 - k : y0 - k + n, :])
            z_term = c * (ext[z + 4 + k, y0 : y0 + n, :] - ext[z + 4 - k, y0 : y0 + n, :])
            gy = y_term if gy is None else gy + y_term
            gz = z_term if gz is None else gz + z_term
        m = jnp.sqrt(gz * gz + gy * gy + gx * gx + 1.0) - 1.0
        mag_ref[z, 8 * t0 : 8 * (t0 + nt), :] = m
        q = jnp.clip(m * (BINS / RANGE), 0.5, BINS - 0.5) - 0.5
        low = jnp.minimum(jnp.floor(q), BINS - 2.0)
        frac = q - low
        w = jnp.clip(jnp.minimum(q - lower, upper - q), 0.0, 1.0)
        wm = w * m
        worst = m + RANGE * (1.0 - w)
        coarse = jnp.floor(low * (1.0 / FINE))
        fine = low - FINE * coarse
        frac_hi = frac.astype(BF16).astype(F32)
        frac_lo = frac - frac_hi
        left, right = [], []
        zero = jnp.zeros((16, 128), BF16)
        one = jnp.ones((16, 128), BF16)
        for i in range(nt):
            s = slice(8 * i, 8 * i + 8)
            c2 = (twice(coarse[s]) - parity).astype(BF16)
            f2 = (twice(fine[s]) - parity).astype(BF16)
            h2 = twice(frac_hi[s]).astype(BF16)
            l2 = twice(frac_lo[s]).astype(BF16)
            ones, his, los = [], [], []
            for j in range(COARSE // 2):
                hit = c2 == jnp.asarray(2 * j, BF16)
                ones.append(jnp.where(hit, one, zero))
                his.append(jnp.where(hit, h2, zero))
                los.append(jnp.where(hit, l2, zero))
            left.append(jnp.concatenate(ones + his + los, axis=0))
            right.append(
                jnp.concatenate(
                    [jnp.where(f2 == jnp.asarray(2 * j, BF16), one, zero) for j in range(FINE // 2)], axis=0
                )
            )
        fold = lambda op, a: functools.reduce(op, [a[8 * i : 8 * i + 8] for i in range(nt)])
        return left, right, fold(jnp.add, wm), fold(jnp.add, w), fold(jnp.maximum, wm), fold(jnp.minimum, worst)

    def several(blocks, carry):
        left, right = [], []
        s, n, hi, lo = carry
        gx = rates(blocks)
        start = 0
        for z, t0, nt in blocks:
            l, r, ps, pn, phi, plo = plane(z, t0, nt, gx[start : start + 8 * nt])
            start += 8 * nt
            left += l
            right += r
            s, n, hi, lo = s + ps, n + pn, jnp.maximum(hi, phi), jnp.minimum(lo, plo)
        acc[...] += lax.dot_general(
            jnp.concatenate(left, axis=1),
            jnp.concatenate(right, axis=1),
            (((1,), (1,)), ((), ())),
            preferred_element_type=F32,
        )
        return s, n, hi, lo

    zeros = jnp.zeros((8, 128), F32)
    carry = (zeros, zeros, zeros, jnp.full((8, 128), 3.0e38, F32))
    tiles = ny // 8
    inner = (nz - 8) // UNROLL
    carry = lax.fori_loop(
        0, inner, lambda t, c: several([(4 + t * UNROLL + u, 1, tiles - 2) for u in range(UNROLL)], c), carry
    )
    y_low.wait()
    y_high.wait()
    ends = [(u, t0, 1) for u in range(nz - 8) for t0 in (0, tiles - 1)]
    carry = lax.fori_loop(
        0, 1, lambda t, c: several([(4 + t * (nz - 8) + u, a, b) for u, a, b in ends], c), carry
    )
    z_low.wait()
    z_high.wait()
    pl.semaphore_wait(ready_y, sizes["gy"] - 1)
    for other in others("gz"):
        pl.semaphore_signal(ready_z, inc=1, device_id={"gz": other}, device_id_type=MESH)

    def edge(t, c):
        z = t * EDGE
        z = z + (z // 4) * (nz - 8)
        return several([(z + u, 0, tiles) for u in range(EDGE)], c)

    wsum, wcount, highest, lowest = lax.fori_loop(0, 8 // EDGE, edge, carry)

    span = COARSE * GROUPS
    rows = lax.broadcasted_iota(jnp.int32, (span, FINE * GROUPS), 0)
    cols = lax.broadcasted_iota(jnp.int32, (span, FINE * GROUPS), 1)
    keep = lax.rem(rows, GROUPS) == lax.rem(cols, GROUPS)

    def by_class(a):
        a = jnp.where(keep, a, 0.0)
        return jnp.sum(a.reshape(COARSE, GROUPS, FINE * GROUPS), axis=1)

    count = by_class(acc[0:span, :])
    part = by_class(acc[span : 2 * span, :] + acc[2 * span : 3 * span, :])
    from_row = lax.broadcasted_iota(jnp.int32, (FINE * GROUPS, 128), 0) // GROUPS
    to_lane = lax.rem(lax.broadcasted_iota(jnp.int32, (FINE * GROUPS, 128), 1), FINE)
    spread = jnp.where(from_row == to_lane, 1.0, 0.0)
    both = jnp.dot(
        jnp.concatenate([count, part], axis=0),
        spread,
        precision=lax.Precision.HIGHEST,
        preferred_element_type=F32,
    )
    r8 = lax.broadcasted_iota(jnp.int32, (16, 128), 0)
    l8 = lax.broadcasted_iota(jnp.int32, (16, 128), 1)
    both = jnp.where(lax.rem(r8, 4) == l8 // FINE, both, 0.0)
    quad = [jnp.sum(both[4 * i : 4 * i + 4], axis=0, keepdims=True) for i in range(4)]
    lane1 = lax.broadcasted_iota(jnp.int32, (1, 128), 1)
    turned = [pltpu.roll(quad[2], 1, 1), pltpu.roll(quad[3], 1, 1)]
    row0 = quad[0] - quad[2] + jnp.where(lane1 == 0, turned[1], turned[0])
    row1 = quad[1] - quad[3] + jnp.where(lane1 == 0, turned[0], turned[1])

    def all_of(op, a):
        return op(op(a, axis=0, keepdims=True), axis=1, keepdims=True)

    row2 = jnp.where(
        lane1 == 0,
        all_of(jnp.min, lowest),
        jnp.where(
            lane1 == 1,
            all_of(jnp.max, highest),
            jnp.where(lane1 == 2, all_of(jnp.sum, wsum), all_of(jnp.sum, wcount)),
        ),
    )
    me = (where["gx"] * sizes["gy"] + where["gy"]) * sizes["gz"] + where["gz"]
    gather[me] = jnp.concatenate([row0, row1, row2, jnp.zeros((1, 128), F32)], axis=0)

    pl.semaphore_wait(ready_z, sizes["gz"] - 1)

    def spread_to(gx, gy, gz):
        pltpu.make_async_remote_copy(
            src_ref=gather.at[me],
            dst_ref=gather.at[me],
            send_sem=all_send,
            recv_sem=all_recv,
            device_id={"gx": gx, "gy": gy, "gz": gz},
            device_id_type=MESH,
        ).start()

    def spread_out(t, c):
        other = lax.rem(me + t, total)
        spread_to(
            other // (sizes["gy"] * sizes["gz"]),
            lax.rem(other // sizes["gz"], sizes["gy"]),
            lax.rem(other, sizes["gz"]),
        )
        return c

    if total > 64:
        lax.fori_loop(1, total, spread_out, 0)
    else:
        far = lambda n: sorted(range(n), key=lambda d: -min(d, n - d))
        for dy in far(sizes["gy"]):
            for dz in far(sizes["gz"]):
                for dx in far(sizes["gx"]):
                    if dx or dy or dz:
                        spread_to(*[ahead[a, d] for a, d in (("gx", dx), ("gy", dy), ("gz", dz))])
    rest = gather.at[pl.ds(0, total - 1)]
    every = pltpu.make_async_remote_copy(
        src_ref=rest,
        dst_ref=rest,
        send_sem=all_send,
        recv_sem=all_recv,
        device_id=up("gx"),
        device_id_type=MESH,
    )
    every.wait()
    parts = gather[...]
    summed = jnp.sum(parts, axis=0)
    smallest = jnp.min(parts, axis=0)
    largest = jnp.max(parts, axis=0)
    cells = nz * ny * nx * total
    hist_ref[...] = summed[0:2] * (BINS / cells)
    stat_ref[...] = jnp.where(
        lane1 == 0,
        smallest[2:3],
        jnp.where(lane1 == 1, largest[2:3], summed[2:3] * (1.0 / cells)),
    )[:, 0:4]


def finish(mag_ref, hist_ref, stat_ref, mag_out, hist_out, stat_out, sem):
    copy = pltpu.make_async_copy(mag_ref, mag_out, sem)
    copy.start()
    hist_out[...] = hist_ref[...]
    stat_out[...] = stat_ref[...]
    copy.wait()


def solution(mesh):
    sizes = dict(mesh.shape)
    total = sizes["gx"] * sizes["gy"] * sizes["gz"]

    def on_device(grid, first, beyond):
        nz, ny, nx = grid.shape
        vmem = pl.BlockSpec(memory_space=pltpu.VMEM)
        hbm = pl.BlockSpec(memory_space=pltpu.HBM)
        packed_rows = nz * ny // 16
        magnitude, histogram, stats = pl.pallas_call(
            functools.partial(kernel, sizes),
            out_shape=(
                jax.ShapeDtypeStruct(grid.shape, F32),
                jax.ShapeDtypeStruct((2, 128), F32),
                jax.ShapeDtypeStruct((1, 4), F32),
            ),
            in_specs=[pl.BlockSpec(memory_space=pltpu.SMEM), pl.BlockSpec(memory_space=pltpu.SMEM), hbm],
            out_specs=(vmem, vmem, vmem),
            scratch_shapes=[
                pltpu.VMEM((nz + 8, ny + 16, nx), F32),
                pltpu.VMEM((packed_rows, 128), F32),
                pltpu.VMEM((packed_rows, 128), F32),
                pltpu.VMEM((packed_rows, 128), F32),
                pltpu.VMEM((256, 128), BF16),
                pltpu.VMEM((256, 2048), BF16),
                pltpu.VMEM((packed_rows, 2048), F32),
                pltpu.VMEM((3 * COARSE * GROUPS, FINE * GROUPS), F32),
                pltpu.VMEM((total, 4, 128), F32),
                pltpu.SemaphoreType.DMA((2,)),
                pltpu.SemaphoreType.DMA((6,)),
                pltpu.SemaphoreType.DMA((6,)),
                pltpu.SemaphoreType.REGULAR,
                pltpu.SemaphoreType.REGULAR,
                pltpu.SemaphoreType.DMA,
                pltpu.SemaphoreType.DMA,
            ],
            compiler_params=pltpu.CompilerParams(
                collective_id=0, has_side_effects=True, vmem_limit_bytes=32768 * 1024
            ),
        )(first, beyond, grid)
        magnitude, histogram, stats = pl.pallas_call(
            finish,
            out_shape=(
                jax.ShapeDtypeStruct(grid.shape, F32),
                jax.ShapeDtypeStruct((2, 128), F32),
                jax.ShapeDtypeStruct((1, 4), F32),
            ),
            in_specs=[vmem, vmem, vmem],
            out_specs=(hbm, vmem, vmem),
            scratch_shapes=[pltpu.SemaphoreType.DMA],
            compiler_params=pltpu.CompilerParams(vmem_limit_bytes=4 * 1024 * 1024),
        )(magnitude, histogram, stats)
        return magnitude, histogram.reshape(BINS), stats.reshape(4)

    return jax.shard_map(
        on_device,
        mesh=mesh,
        in_specs=(P("gz", "gy", "gx"), P(), P()),
        out_specs=(P("gz", "gy", "gx"), P(), P()),
        check_vma=False,
    )
```
